512 devices in a mesh: inp: 32 (over z, x), tm: 16 (over y, core).
Axes of the slice: x: 4, y: 8, z: 8, core: 2. Of those that a mesh axis runs over, the one named last changes fastest.
Arguments:
- samples: bfloat16 [576, 2, 98304], P('inp', None, 'tm'), may hold values from -6 to 6
- delays: int32 [576], P('inp'), may hold values from 0 to 3840
- taps: int32 [16, 256], replicated, may hold values from -2048 to 2047
Outputs:
- visibilities: float32 [256, 576, 1152], P('inp', 'tm')
The draws below stay inside these ranges and needn't reach their ends.
All inputs are finite; a program needn't handle non-finite values.
Results may differ from the reference program's by a relative error of at most 0.0031.
Values may be sent and summed in bfloat16 or wider, within the bound.
No kernel may reach another device: no remote copies, remote signals or barrier semaphores. Data moves between devices by JAX's collectives and lax.ppermute only.
A program may use at most 128 MiB of HBM per device.

```python
import math
import jax
import jax.numpy as jnp
from jax import lax

INPUTS = 576
CH = 256
TAPS = 16
NT = 98304
HALO = 3840


def place_ends(drawn, stream_key, smallest, largest):
    index_at = [jax.random.randint(jax.random.fold_in(stream_key, axis), (), 0, length) for axis, length in enumerate(drawn.shape)]
    main_axis = drawn.shape.index(max(drawn.shape))
    next_to = index_at[:main_axis] + [(index_at[main_axis] + 1) % drawn.shape[main_axis]] + index_at[main_axis + 1:]
    return drawn.at[tuple(index_at)].set(smallest).at[tuple(next_to)].set(largest)


def steps_of(own_key, shape, split, smallest, top_value):
    def one(position, blocks):
        draws = jax.random.uniform(jax.random.fold_in(jax.random.fold_in(own_key, 6), position), (blocks,), jnp.float32, smallest / len(split), top_value / len(split))
        return jnp.repeat(jnp.exp(draws), shape[position] // blocks).reshape((-1,) + (1,) * (len(shape) - position - 1))

    level = one(*split[0])
    for cut in split[1:]:
        level = level * one(*cut)
    return level


def centred(own_key, shape, width, bound, cuts=(), kind=jnp.bfloat16):
    drawn = width * jax.random.normal(own_key, shape, jnp.float32)
    if cuts:
        drawn = drawn * steps_of(own_key, shape, cuts, -0.22, 0.18)
    return jnp.clip(drawn, -bound, bound).astype(kind)


def setup_inputs(seed: int = 0) -> dict:
    arg_keys = jax.random.split(jax.random.key(seed), 4)
    return {
        "samples": centred(arg_keys[0], (INPUTS, 2, NT), 1.0, 6.0, ((0, 32), (2, 16))),
        "delays": place_ends(jax.random.randint(arg_keys[1], (INPUTS,), 0, HALO + 1), jax.random.fold_in(arg_keys[1], 1), 0, HALO).astype(jnp.int32),
        "taps": place_ends(jax.random.randint(arg_keys[2], (TAPS, CH), -2048, 2048), jax.random.fold_in(arg_keys[2], 1), -2048, 2047).astype(jnp.int32),
    }


def dft_table(length):
    channel_index = jnp.arange(length, dtype=jnp.int32)
    phase = (jnp.outer(channel_index, channel_index) % length).astype(jnp.float32) * (2.0 * math.pi / length)
    cosine = jnp.cos(phase)
    sine = jnp.sin(phase)
    upper = jnp.concatenate([cosine, -sine], axis=1)
    lower = jnp.concatenate([sine, cosine], axis=1)
    return jnp.concatenate([upper, lower], axis=0) / math.sqrt(length)

def reference(samples, delays, taps):
    coefficient = taps.astype(jnp.float32) * (1.0 / 4096.0)
    table = dft_table(CH)
    count = NT // CH

    def one_input(operands):
        series, offset = operands
        values = series.astype(jnp.float32)
        aligned = jnp.roll(values, -offset, axis=1)
        frames = aligned.reshape(2, count, CH)
        filtered = jnp.zeros_like(frames)
        for tap in range(TAPS):
            filtered = filtered + coefficient[tap][None, None, :] * jnp.roll(frames, tap, axis=1)
        stacked = jnp.concatenate([filtered[0], filtered[1]], axis=1)
        spectrum = jnp.dot(stacked, table, precision=lax.Precision.HIGHEST)
        return spectrum.astype(jnp.bfloat16)
    spectra = lax.map(one_input, (samples, delays.astype(jnp.int32)))
    by_channel = jnp.transpose(spectra, (2, 0, 1))

    def one_channel(operands):
        real_part, imag_part = operands
        row_block = jnp.concatenate([real_part, imag_part], axis=1)
        swapped = jnp.concatenate([imag_part, -real_part], axis=1)
        gram_real = jnp.dot(row_block, row_block.T, preferred_element_type=jnp.float32)
        gram_imag = jnp.dot(swapped, row_block.T, preferred_element_type=jnp.float32)
        return jnp.concatenate([gram_real, gram_imag], axis=1) * (1.0 / count)
    return lax.map(one_channel, (by_channel[:CH], by_channel[CH:]))
```

```python
import math

import jax
import jax.numpy as jnp
import numpy as np
from jax import lax
from jax.experimental import pallas as pl
from jax.experimental.layout import Layout, with_layout_constraint
from jax.experimental.pallas import tpu as pltpu
from jax.sharding import Mesh
from jax.sharding import PartitionSpec as P

F32 = jnp.float32
BF16 = jnp.bfloat16
LANES = 128
SEG = 18
PER_ROW = 6
HALO_CHUNKS = 32


ORDER = [(p, y) for p in range(32) for y in range(8)]


def split_bf16(value):
    high = value.astype(BF16)
    return high, (value - high.astype(F32)).astype(BF16)


def dft_tables():
    sample = np.arange(128)
    out = []
    for parity in range(2):
        channel = np.array([8 * p + y for p, y in ORDER if y % 2 == parity])
        phase = (np.outer(channel, sample) % 256) * (2.0 * math.pi / 256)
        cosine, sine = np.cos(phase) / 16.0, np.sin(phase) / 16.0
        out.append([np.concatenate([cosine, sine], 1), np.concatenate([-sine, cosine], 1)])
    table = np.asarray(out).reshape(512, 256).astype(np.float32)
    high = table.astype(BF16)
    low = (table - high.astype(np.float32)).astype(BF16)
    return high, low


def filterbank(delays, own, prev, nxt, taps, high, low, out, series, aligned, coef, fir, filt, spec):
    lane = lax.broadcasted_iota(jnp.int32, (160, LANES), 1)
    row8 = lax.broadcasted_iota(jnp.int32, (8, LANES), 0)
    second = (row8 // 2) % 2 == 1
    for tap in range(16):
        first_half = jnp.broadcast_to(taps[pl.ds(tap, 1), :LANES], (8, LANES))
        second_half = jnp.broadcast_to(taps[pl.ds(tap, 1), LANES:], (8, LANES))
        coef[tap] = jnp.where(second, second_half, first_half).astype(F32) * (1.0 / 4096.0)

    def one(i, carry):
        delay = delays[i]
        chunk = delay // LANES
        turn = delay - chunk * LANES
        series[pl.ds(0, 64), :] = prev[pl.ds(pl.multiple_of(i * 64, 64), 64), :].astype(F32)
        series[pl.ds(64, 96), :] = own[pl.ds(pl.multiple_of(i * 96, 32), 96), :].astype(F32)
        series[pl.ds(160, 64), :] = nxt[pl.ds(pl.multiple_of(i * 64, 64), 64), :].astype(F32)
        here = series[pl.ds(4 + 2 * chunk, 160), :]
        after = series[pl.ds(6 + 2 * chunk, 160), :]
        mixed = jnp.where(lane < turn, after, here)
        aligned[...] = pltpu.roll(mixed, (LANES - turn) % LANES, 1)
        total = jnp.zeros((12, 8, LANES), F32)
        for tap in range(16):
            block = aligned[pl.ds(4 * (15 - tap), 96), :].reshape(12, 8, LANES)
            total = total + coef[tap][None] * block
        fir[...] = total.reshape(96, LANES)
        for comp in range(2):
            for k in range(4):
                low_half = fir[pl.ds(24 * k + comp, PER_ROW, stride=4), :]
                high_half = fir[pl.ds(24 * k + 2 + comp, PER_ROW, stride=4), :]
                rows = pl.ds(LANES * k + i, PER_ROW, stride=SEG)
                filt[comp, rows, :] = low_half + high_half
                filt[2 + comp, rows, :] = low_half - high_half
        return carry

    lax.fori_loop(0, SEG, one, 0)
    contract = (((1,), (1,)), ((), ()))
    for k in range(4):
        rows = pl.ds(LANES * k, LANES)
        for parity in range(2):
            values = jnp.concatenate([filt[2 * parity, rows, :], filt[2 * parity + 1, rows, :]], axis=1)
            vh, vl = split_bf16(values)
            th = high[pl.ds(256 * parity, 256), :]
            tl = low[pl.ds(256 * parity, 256), :]
            result = lax.dot_general(th, vh, contract, preferred_element_type=F32)
            result += lax.dot_general(th, vl, contract, preferred_element_type=F32)
            result += lax.dot_general(tl, vh, contract, preferred_element_type=F32)
            for part in range(2):
                start = parity * 8 + part * 4 + k
                spec[pl.ds(start, 128, stride=16), :] = result[128 * part : 128 * part + 128]
    for piece in range(16):
        rows = pl.ds(128 * piece, 128)
        out[rows, :] = spec[rows, :].astype(BF16)[:, :108]


def correlate(half, got, out, sorted_, rows_v, rows_l):
    def arrange(block, carry):
        for pair in range(4):
            message = got[pl.ds(pl.multiple_of(block * 64 + pair * 16, 16), 16), :].astype(F32)
            for e in range(2):
                start = pl.multiple_of(block * 64, 64) + 2 * pair + e
                sorted_[pl.ds(start, 8, stride=8), :108] = message[8 * e : 8 * e + 8]
        return carry

    lax.fori_loop(0, 64, arrange, 0)
    lane = lax.broadcasted_iota(jnp.int32, (8, LANES), 1)
    mine = half[0]

    def build(dst, count, source_of):
        tiles = -(-count * SEG // LANES)

        def one(pk, carry):
            for s in range(PER_ROW):
                blocks = [[None] * tiles for _ in range(2)]
                for core in range(2):
                    for slot in range(count):
                        start = (core * 32 + source_of(slot)) * 64 + pk * 8
                        piece = sorted_[pl.ds(pl.multiple_of(start, 8), 8), :]
                        shift = (SEG * slot - SEG * s) % LANES
                        piece = pltpu.roll(piece, shift, 1) if shift else piece
                        begin, end = SEG * slot, SEG * slot + SEG
                        for tile in range(begin // LANES, (end - 1) // LANES + 1):
                            lo = max(begin - tile * LANES, 0)
                            old = blocks[core][tile]
                            if old is None:
                                blocks[core][tile] = piece
                            else:
                                blocks[core][tile] = jnp.where(lane < lo, old, piece)
                for tile in range(tiles):
                    both = jnp.concatenate([blocks[0][tile], blocks[1][tile]], axis=0).astype(BF16)
                    start = pl.multiple_of((pk * PER_ROW + s) * 16, 16)
                    dst[pl.ds(start, 16), tile * LANES : tile * LANES + LANES] = both
            return carry

        lax.fori_loop(0, 8, one, 0)

    build(rows_v, 32, lambda slot: slot)
    build(rows_l, 16, lambda slot: 4 * (slot // 2) + 2 * mine + slot % 2)
    contract = (((0,), (0,)), ((), ()))

    def product(left, right):
        return lax.dot_general(
            rows_l[pl.ds(384 * left, 384), :], rows_v[pl.ds(384 * right, 384), :], contract, preferred_element_type=F32
        )

    real = (product(0, 0) + product(1, 1))[:288, :576]
    imag = (product(1, 0) - product(0, 1))[:288, :576]
    both = (jnp.concatenate([real, imag], axis=1) * (1.0 / 384.0))
    for block in range(8):
        for tile in range(9):
            out[block, pl.ds(36 * tile, 36), :] = both[
                36 * block : 36 * block + 36, LANES * tile : LANES * tile + LANES
            ].astype(BF16)


def halves(delays, samples, taps):
    chunks = samples.reshape(SEG, 2, 48, LANES).transpose(0, 2, 1, 3)
    perm = lambda by: [(i, (i + by) % 16) for i in range(16)]
    tail = chunks[:, 48 - HALO_CHUNKS :]
    head = chunks[:, :HALO_CHUNKS]
    prev = lax.ppermute(tail, ("y", "core"), perm(1))
    nxt = lax.ppermute(head, ("y", "core"), perm(-1))
    flat = lambda v: v.reshape(-1, LANES)
    return flat(chunks), flat(prev), flat(nxt)


def run_filterbank(delays, own, prev, nxt, taps, interpret=False):
    high, low = dft_tables()
    smem = pl.BlockSpec(memory_space=pltpu.SMEM)
    vmem = pl.BlockSpec(memory_space=pltpu.VMEM)
    return pl.pallas_call(
        filterbank,
        out_shape=jax.ShapeDtypeStruct((2048, 108), BF16),
        in_specs=[smem] + [vmem] * 6,
        out_specs=vmem,
        scratch_shapes=[
            pltpu.VMEM((232, LANES), F32),
            pltpu.VMEM((160, LANES), F32),
            pltpu.VMEM((16, 8, LANES), F32),
            pltpu.VMEM((96, LANES), F32),
            pltpu.VMEM((4, 512, LANES), F32),
            pltpu.VMEM((2048, LANES), F32),
        ],
        compiler_params=pltpu.CompilerParams(vmem_limit_bytes=48 << 20),
        interpret=interpret,
        name="filterbank",
    )(delays, own, prev, nxt, taps, jnp.asarray(high), jnp.asarray(low))


def run_correlate(half, got, interpret=False):
    smem = pl.BlockSpec(memory_space=pltpu.SMEM)
    vmem = pl.BlockSpec(memory_space=pltpu.VMEM)
    return pl.pallas_call(
        correlate,
        out_shape=jax.ShapeDtypeStruct((8, 324, LANES), BF16),
        in_specs=[smem, vmem],
        out_specs=vmem,
        scratch_shapes=[
            pltpu.VMEM((4096, LANES), F32),
            pltpu.VMEM((768, 640), BF16),
            pltpu.VMEM((768, 384), BF16),
        ],
        compiler_params=pltpu.CompilerParams(vmem_limit_bytes=48 << 20),
        interpret=interpret,
        name="correlate",
    )(half, got)


def row_major(value):
    return with_layout_constraint(value, Layout(tuple(range(value.ndim))))


def finish(rows):
    value = rows.reshape(8, 9, 36, LANES).astype(F32)
    return value.transpose(0, 2, 1, 3).reshape(8, 36, 1152)


def shards(samples, delays, taps):
    own, prev, nxt = halves(delays, samples, taps)
    spectra = run_filterbank(delays, own, prev, nxt, taps)
    turned = lax.all_to_all(spectra.reshape(256, 8, 108), ("inp", "y"), 0, 0, tiled=True)
    turned = row_major(turned.reshape(2048, 108))
    both = row_major(lax.all_gather(turned, "core", axis=0, tiled=True))
    half = lax.axis_index("core").astype(jnp.int32).reshape(1)
    rows = run_correlate(half, both)
    mine = lax.all_to_all(rows, "y", 0, 0, tiled=True)
    return finish(mine)


def solution(mesh):
    fine = Mesh(mesh.devices.reshape(32, 8, 2), ("inp", "y", "core"))
    in_specs = (P("inp", None, ("y", "core")), P("inp"), P())
    out_specs = P("inp", ("y", "core"), None)
    return jax.shard_map(shards, mesh=fine, in_specs=in_specs, out_specs=out_specs, check_vma=False)
```

```python
import math

import jax
import jax.numpy as jnp
import numpy as np
from jax import lax
from jax.experimental import pallas as pl
from jax.experimental.layout import Layout, with_layout_constraint
from jax.experimental.pallas import tpu as pltpu
from jax.sharding import Mesh
from jax.sharding import PartitionSpec as P

F32 = jnp.float32
BF16 = jnp.bfloat16
LANES = 128
SEG = 18
PER_ROW = 6
HALO_CHUNKS = 32


ORDER = [(p, y) for p in range(32) for y in range(8)]


def split_bf16(value):
    high = value.astype(BF16)
    return high, (value - high.astype(F32)).astype(BF16)


def dft_tables():
    sample = np.arange(128)
    out = []
    for parity in range(2):
        channel = np.array([8 * p + y for p, y in ORDER if y % 2 == parity])
        phase = (np.outer(channel, sample) % 256) * (2.0 * math.pi / 256)
        cosine, sine = np.cos(phase) / 16.0, np.sin(phase) / 16.0
        out.append([np.concatenate([cosine, sine], 1), np.concatenate([-sine, cosine], 1)])
    table = np.asarray(out).reshape(512, 256).astype(np.float32)
    high = table.astype(BF16)
    low = (table - high.astype(np.float32)).astype(BF16)
    return high, low


def filterbank(delays, own, prev, nxt, taps, high, low, out, series, aligned, coef, fir, filt, spec):
    lane = lax.broadcasted_iota(jnp.int32, (160, LANES), 1)
    row8 = lax.broadcasted_iota(jnp.int32, (8, LANES), 0)
    second = (row8 // 2) % 2 == 1
    for tap in range(16):
        first_half = jnp.broadcast_to(taps[pl.ds(tap, 1), :LANES], (8, LANES))
        second_half = jnp.broadcast_to(taps[pl.ds(tap, 1), LANES:], (8, LANES))
        coef[tap] = jnp.where(second, second_half, first_half)

    def one(i, carry):
        chunk = delays[0, i]
        turn = delays[1, i]
        series[pl.ds(0, 64), :] = prev[pl.ds(pl.multiple_of(i * 64, 64), 64), :].astype(F32)
        series[pl.ds(64, 96), :] = own[pl.ds(pl.multiple_of(i * 96, 32), 96), :].astype(F32)
        series[pl.ds(160, 64), :] = nxt[pl.ds(pl.multiple_of(i * 64, 64), 64), :].astype(F32)
        here = series[pl.ds(4 + 2 * chunk, 160), :]
        after = series[pl.ds(6 + 2 * chunk, 160), :]
        mixed = jnp.where(lane < turn, after, here)
        aligned[...] = pltpu.roll(mixed, (LANES - turn) % LANES, 1)
        total = jnp.zeros((12, 8, LANES), F32)
        for tap in range(16):
            block = aligned[pl.ds(4 * (15 - tap), 96), :].reshape(12, 8, LANES)
            total = total + coef[tap][None] * block
        fir[...] = total.reshape(96, LANES)
        for comp in range(2):
            for k in range(4):
                low_half = fir[pl.ds(24 * k + comp, PER_ROW, stride=4), :]
                high_half = fir[pl.ds(24 * k + 2 + comp, PER_ROW, stride=4), :]
                rows = pl.ds(LANES * k + i, PER_ROW, stride=SEG)
                filt[comp, rows, :] = low_half + high_half
                filt[2 + comp, rows, :] = low_half - high_half
        return carry

    lax.fori_loop(0, SEG, one, 0)
    contract = (((1,), (1,)), ((), ()))
    for k in range(4):
        rows = pl.ds(LANES * k, LANES)
        for parity in range(2):
            values = jnp.concatenate([filt[2 * parity, rows, :], filt[2 * parity + 1, rows, :]], axis=1)
            vh, vl = split_bf16(values)
            th = high[pl.ds(256 * parity, 256), :]
            tl = low[pl.ds(256 * parity, 256), :]
            result = lax.dot_general(th, vh, contract, preferred_element_type=F32)
            result += lax.dot_general(th, vl, contract, preferred_element_type=F32)
            result += lax.dot_general(tl, vh, contract, preferred_element_type=F32)
            for part in range(2):
                start = parity * 8 + part * 4 + k
                spec[pl.ds(start, 128, stride=16), :] = result[128 * part : 128 * part + 128]
    for piece in range(16):
        rows = pl.ds(128 * piece, 128)
        out[rows, :] = spec[rows, :].astype(BF16)[:, :108]


def correlate(half, got, out, rows_v, rows_l):
    lane = lax.broadcasted_iota(jnp.int32, (16, LANES), 1)
    sign = jnp.where(lax.broadcasted_iota(jnp.int32, (8, LANES), 0) < 4, 1.0, -1.0)
    mine = half[0]

    def gather_lanes(dst, group, pieces):
        turned = {}
        for diff in range(1 - PER_ROW, 32):
            merged = None
            for s in range(PER_ROW):
                if 0 <= diff + s < 32:
                    piece = pieces[diff + s]
                    merged = piece if merged is None else jnp.where(lane < SEG * s, merged, piece)
            shift = (SEG * diff) % LANES
            turned[diff] = pltpu.roll(merged, shift, 1) if shift else merged
        for s in range(PER_ROW):
            tiles = [None] * 5
            for slot in range(32):
                begin, end = SEG * slot, SEG * slot + SEG
                for tile in range(begin // LANES, (end - 1) // LANES + 1):
                    new = turned[slot - s]
                    old = tiles[tile]
                    tiles[tile] = new if old is None else jnp.where(lane < begin - tile * LANES, old, new)
            for tile in range(5):
                rows = pl.ds(pl.multiple_of((group * PER_ROW + s) * 16, 16), 16)
                dst[rows, tile * LANES : tile * LANES + LANES] = tiles[tile].astype(BF16)

    def piece_at(group, p):
        core, pair = group // 4, group % 4
        start = pl.multiple_of(core * 2048 + p * 64 + pair * 16, 16)
        return pad(got[pl.ds(start, 16), :])

    def pad(piece):
        return jnp.concatenate([piece, jnp.zeros((16, LANES - 108), BF16)], axis=1)

    def swapped(piece):
        value = piece.astype(F32)
        parts = [pltpu.roll(value[8 * e : 8 * e + 8], 4, 0) * sign for e in range(2)]
        return jnp.concatenate(parts, axis=0).astype(BF16)

    def one(group, carry):
        gather_lanes(rows_v, group, [piece_at(group, p) for p in range(32)])
        own = [piece_at(group, 4 * (u // 2) + 2 * mine + u % 2) for u in range(16)]
        gather_lanes(rows_l, group, own + [swapped(piece) for piece in own])
        return carry

    lax.fori_loop(0, 8, one, 0)
    gram = lax.dot_general(
        rows_l[...], rows_v[...], (((0,), (0,)), ((), ())), preferred_element_type=F32
    ) * (1.0 / 384.0)
    both = jnp.concatenate([gram[:288, :576], gram[288:576, :576]], axis=1)
    for block in range(8):
        for tile in range(9):
            out[block, pl.ds(36 * tile, 36), :] = both[
                36 * block : 36 * block + 36, LANES * tile : LANES * tile + LANES
            ].astype(BF16)


def with_neighbours(samples):
    chunks = samples.reshape(SEG, 2, 48, LANES).transpose(0, 2, 1, 3).reshape(SEG, 96, LANES)
    ring = lambda by: [(i, (i + by) % 16) for i in range(16)]
    prev = lax.ppermute(chunks[:, 32:], ("y", "core"), ring(1))
    nxt = lax.ppermute(chunks[:, :64], ("y", "core"), ring(-1))
    return [v.reshape(-1, LANES) for v in (chunks, prev, nxt)]


def run_filterbank(delays, own, prev, nxt, taps, interpret=False):
    high, low = dft_tables()
    smem = pl.BlockSpec(memory_space=pltpu.SMEM)
    vmem = pl.BlockSpec(memory_space=pltpu.VMEM)
    return pl.pallas_call(
        filterbank,
        out_shape=jax.ShapeDtypeStruct((2048, 108), BF16),
        in_specs=[smem] + [vmem] * 6,
        out_specs=vmem,
        scratch_shapes=[
            pltpu.VMEM((232, LANES), F32),
            pltpu.VMEM((160, LANES), F32),
            pltpu.VMEM((16, 8, LANES), F32),
            pltpu.VMEM((96, LANES), F32),
            pltpu.VMEM((4, 512, LANES), F32),
            pltpu.VMEM((2048, LANES), F32),
        ],
        compiler_params=pltpu.CompilerParams(vmem_limit_bytes=48 << 20),
        interpret=interpret,
        name="filterbank",
    )(delays, own, prev, nxt, taps, jnp.asarray(high), jnp.asarray(low))


def run_correlate(half, got, interpret=False):
    smem = pl.BlockSpec(memory_space=pltpu.SMEM)
    vmem = pl.BlockSpec(memory_space=pltpu.VMEM)
    return pl.pallas_call(
        correlate,
        out_shape=jax.ShapeDtypeStruct((8, 324, LANES), BF16),
        in_specs=[smem, vmem],
        out_specs=vmem,
        scratch_shapes=[
            pltpu.VMEM((768, 640), BF16),
            pltpu.VMEM((768, 640), BF16),
        ],
        compiler_params=pltpu.CompilerParams(vmem_limit_bytes=48 << 20),
        interpret=interpret,
        name="correlate",
    )(half, got)


def row_major(value):
    return with_layout_constraint(value, Layout(tuple(range(value.ndim))))


def finish(rows):
    value = rows.reshape(8, 9, 36, LANES).astype(F32)
    return value.transpose(0, 2, 1, 3).reshape(8, 36, 1152)


def shards(samples, delays, taps):
    own, prev, nxt = with_neighbours(samples)
    split = jnp.stack([delays // LANES, delays % LANES])
    coefficient = taps.astype(F32) * (1.0 / 4096.0)
    spectra = run_filterbank(split, own, prev, nxt, coefficient)
    turned = lax.all_to_all(spectra.reshape(256, 8, 108), ("inp", "y"), 0, 0, tiled=True)
    turned = row_major(turned.reshape(2048, 108))
    both = row_major(lax.all_gather(turned, "core", axis=0, tiled=True))
    half = lax.axis_index("core").astype(jnp.int32).reshape(1)
    rows = run_correlate(half, both)
    mine = lax.all_to_all(rows, "y", 0, 0, tiled=True)
    return finish(mine)


def solution(mesh):
    fine = Mesh(mesh.devices.reshape(32, 8, 2), ("inp", "y", "core"))
    in_specs = (P("inp", None, ("y", "core")), P("inp"), P())
    out_specs = P("inp", ("y", "core"), None)
    return jax.shard_map(shards, mesh=fine, in_specs=in_specs, out_specs=out_specs, check_vma=False)
```

```python
import math

import jax
import jax.numpy as jnp
import numpy as np
from jax import lax
from jax.experimental import pallas as pl
from jax.experimental.layout import Layout, with_layout_constraint
from jax.experimental.pallas import tpu as pltpu
from jax.sharding import Mesh
from jax.sharding import PartitionSpec as P

F32 = jnp.float32
BF16 = jnp.bfloat16
LANES = 128
SEG = 18
PER_ROW = 6
HALO_CHUNKS = 32
AT_ONCE = 6


def exchange_order():
    pairs = [(p, y) for p in range(32) for y in range(0, 8, 2)]
    shuffled = [pairs[i] for i in np.random.RandomState(0).permutation(128)]
    return [(p, y + e) for p, y in shuffled for e in range(2)]


ORDER = exchange_order()
GROUP = [[8 * p + y for p, y in ORDER]]
PAIR_AT = np.asarray([ORDER.index((p, 2 * j)) // 2 for j in range(4) for p in range(32)], np.int32)
ROWS_TO = [0, 3, 6, 1, 4, 7, 2, 5]


def split_bf16(value):
    high = value.astype(BF16)
    return high, (value - high.astype(F32)).astype(BF16)


def dft_tables():
    sample = np.arange(128)
    out = []
    for parity in range(2):
        channel = np.array([8 * p + y for p, y in ORDER if y % 2 == parity])
        phase = (np.outer(channel, sample) % 256) * (2.0 * math.pi / 256)
        cosine, sine = np.cos(phase) / 16.0, np.sin(phase) / 16.0
        out.append([np.concatenate([cosine, sine], 1), np.concatenate([-sine, cosine], 1)])
    table = np.asarray(out).reshape(512, 256).astype(np.float32)
    high = table.astype(BF16)
    low = (table - high.astype(np.float32)).astype(BF16)
    return high, low


def filterbank(delays, own, prev, nxt, taps, high, low, out, series, aligned, coef, fir, filt, spec):
    lane = lax.broadcasted_iota(jnp.int32, (160, LANES), 1)
    row8 = lax.broadcasted_iota(jnp.int32, (8, LANES), 0)
    second = (row8 // 2) % 2 == 1
    for tap in range(16):
        first_half = jnp.broadcast_to(taps[pl.ds(tap, 1), :LANES], (8, LANES))
        second_half = jnp.broadcast_to(taps[pl.ds(tap, 1), LANES:], (8, LANES))
        coef[tap] = jnp.where(second, second_half, first_half)

    def one(i, u):
        chunk = delays[0, i]
        turn = delays[1, i]
        series[u, pl.ds(0, 64), :] = prev[pl.ds(pl.multiple_of(i * 64, 64), 64), :].astype(F32)
        series[u, pl.ds(64, 96), :] = own[pl.ds(pl.multiple_of(i * 96, 32), 96), :].astype(F32)
        series[u, pl.ds(160, 64), :] = nxt[pl.ds(pl.multiple_of(i * 64, 64), 64), :].astype(F32)
        here = series[u, pl.ds(4 + 2 * chunk, 160), :]
        after = series[u, pl.ds(6 + 2 * chunk, 160), :]
        mixed = jnp.where(lane < turn, after, here)
        aligned[u] = pltpu.roll(mixed, (LANES - turn) % LANES, 1)
        total = jnp.zeros((12, 8, LANES), F32)
        for tap in range(16):
            block = aligned[u, pl.ds(4 * (15 - tap), 96), :].reshape(12, 8, LANES)
            total = total + coef[tap][None] * block
        fir[u] = total.reshape(96, LANES)
        for comp in range(2):
            for k in range(4):
                low_half = fir[u, pl.ds(24 * k + comp, PER_ROW, stride=4), :]
                high_half = fir[u, pl.ds(24 * k + 2 + comp, PER_ROW, stride=4), :]
                rows = pl.ds(LANES * k + i, PER_ROW, stride=SEG)
                filt[comp, rows, :] = low_half + high_half
                filt[2 + comp, rows, :] = low_half - high_half

    def some(step, carry):
        for u in range(AT_ONCE):
            one(step * AT_ONCE + u, u)
        return carry

    lax.fori_loop(0, SEG // AT_ONCE, some, 0)
    contract = (((1,), (1,)), ((), ()))
    for k in range(4):
        rows = pl.ds(LANES * k, LANES)
        for parity in range(2):
            values = jnp.concatenate([filt[2 * parity, rows, :], filt[2 * parity + 1, rows, :]], axis=1)
            vh, vl = split_bf16(values)
            th = high[pl.ds(256 * parity, 256), :]
            tl = low[pl.ds(256 * parity, 256), :]
            result = lax.dot_general(th, vh, contract, preferred_element_type=F32)
            result += lax.dot_general(th, vl, contract, preferred_element_type=F32)
            result += lax.dot_general(tl, vh, contract, preferred_element_type=F32)
            for part in range(2):
                start = parity * 8 + part * 4 + k
                spec[pl.ds(start, 128, stride=16), :] = result[128 * part : 128 * part + 128]
    for piece in range(16):
        rows = pl.ds(128 * piece, 128)
        out[rows, :] = spec[rows, :].astype(BF16)[:, :108]


def correlate(half, pair_at, got, out, rows_v, rows_l):
    lane = lax.broadcasted_iota(jnp.int32, (16, LANES), 1)
    sign = jnp.where(lax.broadcasted_iota(jnp.int32, (8, LANES), 0) < 4, 1.0, -1.0)
    mine = half[0]

    def gather_lanes(dst, group, pieces):
        turned = {}
        for diff in range(1 - PER_ROW, 32):
            merged = None
            for s in range(PER_ROW):
                if 0 <= diff + s < 32:
                    piece = pieces[diff + s]
                    merged = piece if merged is None else jnp.where(lane < SEG * s, merged, piece)
            shift = (SEG * diff) % LANES
            turned[diff] = pltpu.roll(merged, shift, 1) if shift else merged
        for s in range(PER_ROW):
            tiles = [None] * 5
            for slot in range(32):
                begin, end = SEG * slot, SEG * slot + SEG
                for tile in range(begin // LANES, (end - 1) // LANES + 1):
                    new = turned[slot - s]
                    old = tiles[tile]
                    tiles[tile] = new if old is None else jnp.where(lane < begin - tile * LANES, old, new)
            for tile in range(5):
                rows = pl.ds(pl.multiple_of((group * PER_ROW + s) * 16, 16), 16)
                dst[rows, tile * LANES : tile * LANES + LANES] = tiles[tile].astype(BF16)

    def piece_at(group, p):
        core, pair = group // 4, group % 4
        start = pl.multiple_of(core * 2048 + pair_at[pair * 32 + p] * 16, 16)
        return pad(got[pl.ds(start, 16), :])

    def pad(piece):
        return jnp.concatenate([piece, jnp.zeros((16, LANES - 108), BF16)], axis=1)

    def swapped(piece):
        value = piece.astype(F32)
        parts = [pltpu.roll(value[8 * e : 8 * e + 8], 4, 0) * sign for e in range(2)]
        return jnp.concatenate(parts, axis=0).astype(BF16)

    def one(group, carry):
        gather_lanes(rows_v, group, [piece_at(group, p) for p in range(32)])
        own = [piece_at(group, 4 * (u // 2) + 2 * mine + u % 2) for u in range(16)]
        gather_lanes(rows_l, group, own + [swapped(piece) for piece in own])
        return carry

    lax.fori_loop(0, 8, one, 0)
    gram = lax.dot_general(
        rows_l[...], rows_v[...], (((0,), (0,)), ((), ())), preferred_element_type=F32
    ) * (1.0 / 384.0)
    both = jnp.concatenate([gram[:288, :576], gram[288:576, :576]], axis=1)
    for place, block in enumerate(ROWS_TO):
        for tile in range(9):
            out[place, pl.ds(36 * tile, 36), :] = both[
                36 * block : 36 * block + 36, LANES * tile : LANES * tile + LANES
            ].astype(BF16)


def with_neighbours(samples):
    chunks = samples.reshape(SEG, 2, 48, LANES).transpose(0, 2, 1, 3).reshape(SEG, 96, LANES)
    ring = lambda by: [(i, (i + by) % 16) for i in range(16)]
    prev = lax.ppermute(chunks[:, 32:], ("y", "core"), ring(1))
    nxt = lax.ppermute(chunks[:, :64], ("y", "core"), ring(-1))
    return [v.reshape(-1, LANES) for v in (chunks, prev, nxt)]


def run_filterbank(delays, own, prev, nxt, taps, interpret=False):
    high, low = dft_tables()
    smem = pl.BlockSpec(memory_space=pltpu.SMEM)
    vmem = pl.BlockSpec(memory_space=pltpu.VMEM)
    return pl.pallas_call(
        filterbank,
        out_shape=jax.ShapeDtypeStruct((2048, 108), BF16),
        in_specs=[smem] + [vmem] * 6,
        out_specs=vmem,
        scratch_shapes=[
            pltpu.VMEM((AT_ONCE, 232, LANES), F32),
            pltpu.VMEM((AT_ONCE, 160, LANES), F32),
            pltpu.VMEM((16, 8, LANES), F32),
            pltpu.VMEM((AT_ONCE, 96, LANES), F32),
            pltpu.VMEM((4, 512, LANES), F32),
            pltpu.VMEM((2048, LANES), F32),
        ],
        compiler_params=pltpu.CompilerParams(vmem_limit_bytes=48 << 20),
        interpret=interpret,
        name="filterbank",
    )(delays, own, prev, nxt, taps, jnp.asarray(high), jnp.asarray(low))


def run_correlate(half, pair_at, got, interpret=False):
    smem = pl.BlockSpec(memory_space=pltpu.SMEM)
    vmem = pl.BlockSpec(memory_space=pltpu.VMEM)
    return pl.pallas_call(
        correlate,
        out_shape=jax.ShapeDtypeStruct((8, 324, LANES), BF16),
        in_specs=[smem, smem, vmem],
        out_specs=vmem,
        scratch_shapes=[
            pltpu.VMEM((768, 640), BF16),
            pltpu.VMEM((768, 640), BF16),
        ],
        compiler_params=pltpu.CompilerParams(vmem_limit_bytes=48 << 20),
        interpret=interpret,
        name="correlate",
    )(half, pair_at, got)


def row_major(value):
    return with_layout_constraint(value, Layout(tuple(range(value.ndim))))


def finish(rows):
    rows = jnp.stack([rows[ROWS_TO.index(channel)] for channel in range(8)])
    value = rows.reshape(8, 9, 36, LANES).astype(F32)
    return value.transpose(0, 2, 1, 3).reshape(8, 36, 1152)


def shards(samples, delays, taps):
    own, prev, nxt = with_neighbours(samples)
    half = lax.axis_index("core").astype(jnp.int32).reshape(1)
    split = jnp.stack([delays // LANES, delays % LANES])
    split, half, pair_at = lax.optimization_barrier((split, half, jnp.asarray(PAIR_AT)))
    coefficient = taps.astype(F32) * (1.0 / 4096.0)
    spectra = run_filterbank(split, own, prev, nxt, coefficient)
    turned = lax.all_to_all(spectra.reshape(256, 8, 108), ("inp", "y"), 0, 0, axis_index_groups=GROUP, tiled=True)
    turned = row_major(turned.reshape(2048, 108))
    both = row_major(lax.all_gather(turned, "core", axis=0, tiled=True))
    rows = run_correlate(half, pair_at, both)
    mine = lax.all_to_all(rows, "y", 0, 0, axis_index_groups=[ROWS_TO], tiled=True)
    return finish(mine)


def solution(mesh):
    fine = Mesh(mesh.devices.reshape(32, 8, 2), ("inp", "y", "core"))
    in_specs = (P("inp", None, ("y", "core")), P("inp"), P())
    out_specs = P("inp", ("y", "core"), None)
    return jax.shard_map(shards, mesh=fine, in_specs=in_specs, out_specs=out_specs, check_vma=False)
```

```python
import math

import jax
import jax.numpy as jnp
import numpy as np
from jax import lax
from jax.experimental import pallas as pl
from jax.experimental.layout import Layout, with_layout_constraint
from jax.experimental.pallas import tpu as pltpu
from jax.sharding import Mesh
from jax.sharding import PartitionSpec as P

F32 = jnp.float32
BF16 = jnp.bfloat16
LANES = 128
SEG = 18
PER_ROW = 6
HALO_CHUNKS = 32
AT_ONCE = 6


def exchange_order():
    rng = np.random.RandomState(0)
    even = [(p, y) for p in range(32) for y in range(0, 8, 2)]
    odd = [(p, y + 1) for p, y in even]
    even = [even[i] for i in rng.permutation(128)]
    odd = [odd[i] for i in rng.permutation(128)]
    return [chip for both in zip(even, odd) for chip in both]


ORDER = exchange_order()
GROUP = [[8 * p + y for p, y in ORDER]]


def split_bf16(value):
    high = value.astype(BF16)
    return high, (value - high.astype(F32)).astype(BF16)


def dft_tables():
    sample = np.arange(128)
    out = []
    for parity in range(2):
        channel = np.array([8 * p + y for p, y in ORDER if y % 2 == parity])
        phase = (np.outer(channel, sample) % 256) * (2.0 * math.pi / 256)
        cosine, sine = np.cos(phase) / 16.0, np.sin(phase) / 16.0
        out.append([np.concatenate([cosine, sine], 1), np.concatenate([-sine, cosine], 1)])
    table = np.asarray(out).reshape(512, 256).astype(np.float32)
    high = table.astype(BF16)
    low = (table - high.astype(np.float32)).astype(BF16)
    return high, low


def filterbank(delays, own, prev, nxt, taps, high, low, out, series, aligned, coef, fir, filt, spec):
    lane = lax.broadcasted_iota(jnp.int32, (160, LANES), 1)
    row8 = lax.broadcasted_iota(jnp.int32, (8, LANES), 0)
    second = (row8 // 2) % 2 == 1
    for tap in range(16):
        first_half = jnp.broadcast_to(taps[pl.ds(tap, 1), :LANES], (8, LANES))
        second_half = jnp.broadcast_to(taps[pl.ds(tap, 1), LANES:], (8, LANES))
        coef[tap] = jnp.where(second, second_half, first_half)

    def one(i, u):
        chunk = delays[0, i]
        turn = delays[1, i]
        series[u, pl.ds(0, 64), :] = prev[pl.ds(pl.multiple_of(i * 64, 64), 64), :].astype(F32)
        series[u, pl.ds(64, 96), :] = own[pl.ds(pl.multiple_of(i * 96, 32), 96), :].astype(F32)
        series[u, pl.ds(160, 64), :] = nxt[pl.ds(pl.multiple_of(i * 64, 64), 64), :].astype(F32)
        here = series[u, pl.ds(4 + 2 * chunk, 160), :]
        after = series[u, pl.ds(6 + 2 * chunk, 160), :]
        mixed = jnp.where(lane < turn, after, here)
        aligned[u] = pltpu.roll(mixed, (LANES - turn) % LANES, 1)
        total = jnp.zeros((12, 8, LANES), F32)
        for tap in range(16):
            block = aligned[u, pl.ds(4 * (15 - tap), 96), :].reshape(12, 8, LANES)
            total = total + coef[tap][None] * block
        fir[u] = total.reshape(96, LANES)
        for comp in range(2):
            for k in range(4):
                low_half = fir[u, pl.ds(24 * k + comp, PER_ROW, stride=4), :]
                high_half = fir[u, pl.ds(24 * k + 2 + comp, PER_ROW, stride=4), :]
                rows = pl.ds(LANES * k + i, PER_ROW, stride=SEG)
                filt[comp, rows, :] = low_half + high_half
                filt[2 + comp, rows, :] = low_half - high_half

    def some(step, carry):
        for u in range(AT_ONCE):
            one(step * AT_ONCE + u, u)
        return carry

    lax.fori_loop(0, SEG // AT_ONCE, some, 0)
    contract = (((1,), (1,)), ((), ()))
    for wide in range(2):
        rows = pl.ds(2 * LANES * wide, 2 * LANES)
        for parity in range(2):
            values = jnp.concatenate([filt[2 * parity, rows, :], filt[2 * parity + 1, rows, :]], axis=1)
            vh, vl = split_bf16(values)
            th = high[pl.ds(256 * parity, 256), :]
            tl = low[pl.ds(256 * parity, 256), :]
            result = lax.dot_general(th, vh, contract, preferred_element_type=F32)
            result += lax.dot_general(th, vl, contract, preferred_element_type=F32)
            result += lax.dot_general(tl, vh, contract, preferred_element_type=F32)
            for part in range(2):
                for side in range(2):
                    start = parity * 8 + part * 4 + 2 * wide + side
                    spec[pl.ds(start, 128, stride=16), :] = result[
                        128 * part : 128 * part + 128, LANES * side : LANES * side + LANES
                    ]
    for piece in range(16):
        rows = pl.ds(128 * piece, 128)
        out[rows, :] = spec[rows, :].astype(BF16)[:, :108]


def correlate(half, got, out, ranked, rows_v, rows_l):
    lane = lax.broadcasted_iota(jnp.int32, (16, LANES), 1)
    sign = jnp.where(lax.broadcasted_iota(jnp.int32, (8, LANES), 0) < 4, 1.0, -1.0)
    mine = half[0]

    def gather_lanes(dst, group, pieces):
        turned = {}
        for diff in range(1 - PER_ROW, 32):
            merged = None
            for s in range(PER_ROW):
                if 0 <= diff + s < 32:
                    piece = pieces[diff + s]
                    merged = piece if merged is None else jnp.where(lane < SEG * s, merged, piece)
            shift = (SEG * diff) % LANES
            turned[diff] = pltpu.roll(merged, shift, 1) if shift else merged
        for s in range(PER_ROW):
            tiles = [None] * 5
            for slot in range(32):
                begin, end = SEG * slot, SEG * slot + SEG
                for tile in range(begin // LANES, (end - 1) // LANES + 1):
                    new = turned[slot - s]
                    old = tiles[tile]
                    tiles[tile] = new if old is None else jnp.where(lane < begin - tile * LANES, old, new)
            for tile in range(5):
                rows = pl.ds(pl.multiple_of((group * PER_ROW + s) * 16, 16), 16)
                dst[rows, tile * LANES : tile * LANES + LANES] = tiles[tile].astype(BF16)

    def pad(piece):
        return jnp.concatenate([piece, jnp.zeros((16, LANES - 108), BF16)], axis=1)

    for core in range(2):
        for pair in range(128):
            places = [core * 256 + ORDER.index((pair // 4, 2 * (pair % 4) + e)) for e in range(2)]
            both = jnp.concatenate([got[pl.ds(8 * place, 8), :] for place in places], axis=0)
            ranked[pl.ds(core * 2048 + 16 * pair, 16), :] = pad(both)

    def piece_at(group, p):
        core, pair = group // 4, group % 4
        start = pl.multiple_of(core * 2048 + p * 64 + pair * 16, 16)
        return ranked[pl.ds(start, 16), :]

    def swapped(piece):
        value = piece.astype(F32)
        parts = [pltpu.roll(value[8 * e : 8 * e + 8], 4, 0) * sign for e in range(2)]
        return jnp.concatenate(parts, axis=0).astype(BF16)

    def one(group, carry):
        gather_lanes(rows_v, group, [piece_at(group, p) for p in range(32)])
        own = [piece_at(group, 4 * (u // 2) + 2 * mine + u % 2) for u in range(16)]
        gather_lanes(rows_l, group, own + [swapped(piece) for piece in own])
        return carry

    lax.fori_loop(0, 8, one, 0)
    gram = lax.dot_general(
        rows_l[:, :576], rows_v[...], (((0,), (0,)), ((), ())), preferred_element_type=F32
    ) * (1.0 / 384.0)
    both = jnp.concatenate([gram[:288, :576], gram[288:576, :576]], axis=1)
    for block in range(8):
        for tile in range(9):
            out[block, pl.ds(36 * tile, 36), :] = both[
                36 * block : 36 * block + 36, LANES * tile : LANES * tile + LANES
            ].astype(BF16)


def with_neighbours(samples):
    chunks = samples.reshape(SEG, 2, 48, LANES).transpose(0, 2, 1, 3).reshape(SEG, 96, LANES)
    ring = lambda by: [(i, (i + by) % 16) for i in range(16)]
    prev = lax.ppermute(chunks[:, 32:], ("y", "core"), ring(1))
    nxt = lax.ppermute(chunks[:, :64], ("y", "core"), ring(-1))
    return [v.reshape(-1, LANES) for v in (chunks, prev, nxt)]


def run_filterbank(delays, own, prev, nxt, taps, interpret=False):
    high, low = dft_tables()
    smem = pl.BlockSpec(memory_space=pltpu.SMEM)
    vmem = pl.BlockSpec(memory_space=pltpu.VMEM)
    return pl.pallas_call(
        filterbank,
        out_shape=jax.ShapeDtypeStruct((2048, 108), BF16),
        in_specs=[smem] + [vmem] * 6,
        out_specs=vmem,
        scratch_shapes=[
            pltpu.VMEM((AT_ONCE, 232, LANES), F32),
            pltpu.VMEM((AT_ONCE, 160, LANES), F32),
            pltpu.VMEM((16, 8, LANES), F32),
            pltpu.VMEM((AT_ONCE, 96, LANES), F32),
            pltpu.VMEM((4, 512, LANES), F32),
            pltpu.VMEM((2048, LANES), F32),
        ],
        compiler_params=pltpu.CompilerParams(vmem_limit_bytes=48 << 20),
        interpret=interpret,
        name="filterbank",
    )(delays, own, prev, nxt, taps, jnp.asarray(high), jnp.asarray(low))


def run_correlate(half, got, interpret=False):
    smem = pl.BlockSpec(memory_space=pltpu.SMEM)
    vmem = pl.BlockSpec(memory_space=pltpu.VMEM)
    return pl.pallas_call(
        correlate,
        out_shape=jax.ShapeDtypeStruct((8, 324, LANES), BF16),
        in_specs=[smem, vmem],
        out_specs=vmem,
        scratch_shapes=[
            pltpu.VMEM((4096, LANES), BF16),
            pltpu.VMEM((768, 640), BF16),
            pltpu.VMEM((768, 640), BF16),
        ],
        compiler_params=pltpu.CompilerParams(vmem_limit_bytes=48 << 20),
        interpret=interpret,
        name="correlate",
    )(half, got)


def row_major(value):
    return with_layout_constraint(value, Layout(tuple(range(value.ndim))))


def finish(rows):
    value = rows.reshape(8, 9, 36, LANES).astype(F32)
    return value.transpose(0, 2, 1, 3).reshape(8, 36, 1152)


def shards(samples, delays, taps):
    own, prev, nxt = with_neighbours(samples)
    half = lax.axis_index("core").astype(jnp.int32).reshape(1)
    split = jnp.stack([delays // LANES, delays % LANES])
    split, half = lax.optimization_barrier((split, half))
    coefficient = taps.astype(F32) * (1.0 / 4096.0)
    spectra = run_filterbank(split, own, prev, nxt, coefficient)
    turned = lax.all_to_all(spectra.reshape(256, 8, 108), ("inp", "y"), 0, 0, axis_index_groups=GROUP, tiled=True)
    turned = row_major(turned.reshape(2048, 108))
    both = row_major(lax.all_gather(turned, "core", axis=0, tiled=True))
    rows = run_correlate(half, both)
    mine = lax.all_to_all(rows, "y", 0, 0, tiled=True)
    return finish(mine)


def solution(mesh):
    fine = Mesh(mesh.devices.reshape(32, 8, 2), ("inp", "y", "core"))
    in_specs = (P("inp", None, ("y", "core")), P("inp"), P())
    out_specs = P("inp", ("y", "core"), None)
    return jax.shard_map(shards, mesh=fine, in_specs=in_specs, out_specs=out_specs, check_vma=False)
```

```python
import math

import jax
import jax.numpy as jnp
import numpy as np
from jax import lax
from jax.experimental import pallas as pl
from jax.experimental.layout import Layout, with_layout_constraint
from jax.experimental.pallas import tpu as pltpu
from jax.sharding import Mesh
from jax.sharding import PartitionSpec as P

F32 = jnp.float32
BF16 = jnp.bfloat16
LANES = 128
SEG = 18
PER_ROW = 6
HALO_CHUNKS = 32
AT_ONCE = 6


def exchange_order():
    rng = np.random.RandomState(1)
    even = [(p, y) for p in range(32) for y in range(0, 8, 2)]
    odd = [(p, y + 1) for p, y in even]
    even = [even[i] for i in rng.permutation(128)]
    odd = [odd[i] for i in rng.permutation(128)]
    return [chip for both in zip(even, odd) for chip in both]


ORDER = exchange_order()
GROUP = [[8 * p + y for p, y in ORDER]]


def split_bf16(value):
    high = value.astype(BF16)
    return high, (value - high.astype(F32)).astype(BF16)


def dft_tables():
    sample = np.arange(128)
    out = []
    for parity in range(2):
        channel = np.array([8 * p + y for p, y in ORDER if y % 2 == parity])
        phase = (np.outer(channel, sample) % 256) * (2.0 * math.pi / 256)
        cosine, sine = np.cos(phase) / 16.0, np.sin(phase) / 16.0
        out.append([np.concatenate([cosine, sine], 1), np.concatenate([-sine, cosine], 1)])
    table = np.asarray(out).reshape(512, 256).astype(np.float32)
    high = table.astype(BF16)
    low = (table - high.astype(np.float32)).astype(BF16)
    return high, low


def filterbank(delays, own, prev, nxt, taps, high, low, out, series, aligned, coef, fir, filt, spec):
    lane = lax.broadcasted_iota(jnp.int32, (160, LANES), 1)
    row8 = lax.broadcasted_iota(jnp.int32, (8, LANES), 0)
    second = (row8 // 2) % 2 == 1
    for tap in range(16):
        first_half = jnp.broadcast_to(taps[pl.ds(tap, 1), :LANES], (8, LANES))
        second_half = jnp.broadcast_to(taps[pl.ds(tap, 1), LANES:], (8, LANES))
        coef[tap] = jnp.where(second, second_half, first_half)

    def one(i, u):
        chunk = delays[0, i]
        turn = delays[1, i]
        series[u, pl.ds(0, 64), :] = prev[pl.ds(pl.multiple_of(i * 64, 64), 64), :].astype(F32)
        series[u, pl.ds(64, 96), :] = own[pl.ds(pl.multiple_of(i * 96, 32), 96), :].astype(F32)
        series[u, pl.ds(160, 64), :] = nxt[pl.ds(pl.multiple_of(i * 64, 64), 64), :].astype(F32)
        here = series[u, pl.ds(4 + 2 * chunk, 160), :]
        after = series[u, pl.ds(6 + 2 * chunk, 160), :]
        mixed = jnp.where(lane < turn, after, here)
        aligned[u] = pltpu.roll(mixed, (LANES - turn) % LANES, 1)
        total = jnp.zeros((12, 8, LANES), F32)
        for tap in range(16):
            block = aligned[u, pl.ds(4 * (15 - tap), 96), :].reshape(12, 8, LANES)
            total = total + coef[tap][None] * block
        fir[u] = total.reshape(96, LANES)
        for comp in range(2):
            for k in range(4):
                low_half = fir[u, pl.ds(24 * k + comp, PER_ROW, stride=4), :]
                high_half = fir[u, pl.ds(24 * k + 2 + comp, PER_ROW, stride=4), :]
                rows = pl.ds(LANES * k + i, PER_ROW, stride=SEG)
                filt[comp, rows, :] = low_half + high_half
                filt[2 + comp, rows, :] = low_half - high_half

    def some(step, carry):
        for u in range(AT_ONCE):
            one(step * AT_ONCE + u, u)
        return carry

    lax.fori_loop(0, SEG // AT_ONCE, some, 0)
    contract = (((1,), (1,)), ((), ()))
    for wide in range(2):
        rows = pl.ds(2 * LANES * wide, 2 * LANES)
        for parity in range(2):
            values = jnp.concatenate([filt[2 * parity, rows, :], filt[2 * parity + 1, rows, :]], axis=1)
            vh, vl = split_bf16(values)
            th = high[pl.ds(256 * parity, 256), :]
            tl = low[pl.ds(256 * parity, 256), :]
            result = lax.dot_general(th, vh, contract, preferred_element_type=F32)
            result += lax.dot_general(th, vl, contract, preferred_element_type=F32)
            result += lax.dot_general(tl, vh, contract, preferred_element_type=F32)
            for part in range(2):
                for side in range(2):
                    start = parity * 8 + part * 4 + 2 * wide + side
                    spec[pl.ds(start, 128, stride=16), :] = result[
                        128 * part : 128 * part + 128, LANES * side : LANES * side + LANES
                    ]
    for piece in range(16):
        rows = pl.ds(128 * piece, 128)
        out[rows, :] = spec[rows, :].astype(BF16)[:, :108]


def correlate(half, got, out, ranked, rows_v, rows_l):
    lane = lax.broadcasted_iota(jnp.int32, (16, LANES), 1)
    sign = jnp.where(lax.broadcasted_iota(jnp.int32, (8, LANES), 0) < 4, 1.0, -1.0)
    mine = half[0]

    def gather_lanes(dst, group, pieces):
        turned = {}
        for diff in range(1 - PER_ROW, 32):
            merged = None
            for s in range(PER_ROW):
                if 0 <= diff + s < 32:
                    piece = pieces[diff + s]
                    merged = piece if merged is None else jnp.where(lane < SEG * s, merged, piece)
            shift = (SEG * diff) % LANES
            turned[diff] = pltpu.roll(merged, shift, 1) if shift else merged
        for s in range(PER_ROW):
            tiles = [None] * 5
            for slot in range(32):
                begin, end = SEG * slot, SEG * slot + SEG
                for tile in range(begin // LANES, (end - 1) // LANES + 1):
                    new = turned[slot - s]
                    old = tiles[tile]
                    tiles[tile] = new if old is None else jnp.where(lane < begin - tile * LANES, old, new)
            for tile in range(5):
                rows = pl.ds(pl.multiple_of((group * PER_ROW + s) * 16, 16), 16)
                dst[rows, tile * LANES : tile * LANES + LANES] = tiles[tile].astype(BF16)

    def pad(piece):
        return jnp.concatenate([piece, jnp.zeros((16, LANES - 108), BF16)], axis=1)

    for core in range(2):
        for pair in range(128):
            places = [core * 256 + ORDER.index((pair // 4, 2 * (pair % 4) + e)) for e in range(2)]
            both = jnp.concatenate([got[pl.ds(8 * place, 8), :] for place in places], axis=0)
            ranked[pl.ds(core * 2048 + 16 * pair, 16), :] = pad(both)

    def piece_at(group, p):
        core, pair = group // 4, group % 4
        start = pl.multiple_of(core * 2048 + p * 64 + pair * 16, 16)
        return ranked[pl.ds(start, 16), :]

    def swapped(piece):
        value = piece.astype(F32)
        parts = [pltpu.roll(value[8 * e : 8 * e + 8], 4, 0) * sign for e in range(2)]
        return jnp.concatenate(parts, axis=0).astype(BF16)

    def one(group, carry):
        gather_lanes(rows_v, group, [piece_at(group, p) for p in range(32)])
        own = [piece_at(group, 4 * (u // 2) + 2 * mine + u % 2) for u in range(16)]
        gather_lanes(rows_l, group, own + [swapped(piece) for piece in own])
        return carry

    lax.fori_loop(0, 8, one, 0)
    gram = lax.dot_general(
        rows_l[:, :576], rows_v[...], (((0,), (0,)), ((), ())), preferred_element_type=F32
    ) * (1.0 / 384.0)
    both = jnp.concatenate([gram[:288, :576], gram[288:576, :576]], axis=1)
    for block in range(8):
        for tile in range(9):
            out[block, pl.ds(36 * tile, 36), :] = both[
                36 * block : 36 * block + 36, LANES * tile : LANES * tile + LANES
            ].astype(BF16)


def with_neighbours(samples):
    chunks = samples.reshape(SEG, 2, 48, LANES).transpose(0, 2, 1, 3).reshape(SEG, 96, LANES)
    ring = lambda by: [(i, (i + by) % 16) for i in range(16)]
    prev = lax.ppermute(chunks[:, 32:], ("y", "core"), ring(1))
    nxt = lax.ppermute(chunks[:, :64], ("y", "core"), ring(-1))
    return [v.reshape(-1, LANES) for v in (chunks, prev, nxt)]


def run_filterbank(delays, own, prev, nxt, taps, interpret=False):
    high, low = dft_tables()
    smem = pl.BlockSpec(memory_space=pltpu.SMEM)
    vmem = pl.BlockSpec(memory_space=pltpu.VMEM)
    return pl.pallas_call(
        filterbank,
        out_shape=jax.ShapeDtypeStruct((2048, 108), BF16),
        in_specs=[smem] + [vmem] * 6,
        out_specs=vmem,
        scratch_shapes=[
            pltpu.VMEM((AT_ONCE, 232, LANES), F32),
            pltpu.VMEM((AT_ONCE, 160, LANES), F32),
            pltpu.VMEM((16, 8, LANES), F32),
            pltpu.VMEM((AT_ONCE, 96, LANES), F32),
            pltpu.VMEM((4, 512, LANES), F32),
            pltpu.VMEM((2048, LANES), F32),
        ],
        compiler_params=pltpu.CompilerParams(vmem_limit_bytes=48 << 20),
        interpret=interpret,
        name="filterbank",
    )(delays, own, prev, nxt, taps, jnp.asarray(high), jnp.asarray(low))


def run_correlate(half, got, interpret=False):
    smem = pl.BlockSpec(memory_space=pltpu.SMEM)
    vmem = pl.BlockSpec(memory_space=pltpu.VMEM)
    return pl.pallas_call(
        correlate,
        out_shape=jax.ShapeDtypeStruct((8, 324, LANES), BF16),
        in_specs=[smem, vmem],
        out_specs=vmem,
        scratch_shapes=[
            pltpu.VMEM((4096, LANES), BF16),
            pltpu.VMEM((768, 640), BF16),
            pltpu.VMEM((768, 640), BF16),
        ],
        compiler_params=pltpu.CompilerParams(vmem_limit_bytes=48 << 20),
        interpret=interpret,
        name="correlate",
    )(half, got)


def row_major(value):
    return with_layout_constraint(value, Layout(tuple(range(value.ndim))))


def finish(rows):
    value = rows.reshape(8, 9, 36, LANES).astype(F32)
    return value.transpose(0, 2, 1, 3).reshape(8, 36, 1152)


def shards(samples, delays, taps):
    own, prev, nxt = with_neighbours(samples)
    half = lax.axis_index("core").astype(jnp.int32).reshape(1)
    split = jnp.stack([delays // LANES, delays % LANES])
    split, half = lax.optimization_barrier((split, half))
    coefficient = taps.astype(F32) * (1.0 / 4096.0)
    spectra = run_filterbank(split, own, prev, nxt, coefficient)
    turned = lax.all_to_all(spectra.reshape(256, 8, 108), ("inp", "y"), 0, 0, axis_index_groups=GROUP, tiled=True)
    turned = row_major(turned.reshape(2048, 108))
    both = row_major(lax.all_gather(turned, "core", axis=0, tiled=True))
    rows = run_correlate(half, both)
    mine = lax.all_to_all(rows, "y", 0, 0, tiled=True)
    return finish(mine)


def solution(mesh):
    fine = Mesh(mesh.devices.reshape(32, 8, 2), ("inp", "y", "core"))
    in_specs = (P("inp", None, ("y", "core")), P("inp"), P())
    out_specs = P("inp", ("y", "core"), None)
    return jax.shard_map(shards, mesh=fine, in_specs=in_specs, out_specs=out_specs, check_vma=False)
```
